8 devices in a mesh: part: 1 (over z), row: 2 (over y), col: 2 (over x), dep: 2 (over core).
Axes of the slice: x: 2, y: 2, z: 1, core: 2. Of those that a mesh axis runs over, the one named last changes fastest.
Arguments:
- x_in: bfloat16 [4096, 5120], P(('part', 'row', 'col'), 'dep')
- ln_scale: float32 [5120], P('dep')
- ln_shift: float32 [5120], P('dep')
- w_up: bfloat16 [5120, 20480], P(('dep', 'row'), 'col')
- b_up: bfloat16 [20480], P('col')
- w_down: bfloat16 [20480, 5120], P(('col', 'row'), 'dep')
- b_down: bfloat16 [5120], P('dep')
- y_grad: bfloat16 [4096, 5120], P(('part', 'row', 'col'), 'dep')
Outputs:
- output 1: bfloat16 [4096, 5120], P(('part', 'row', 'col'), 'dep')
- output 2: bfloat16 [4096, 5120], P(('part', 'row', 'col'), 'dep')
- output 3: bfloat16 [5120, 20480], P(('part', 'dep', 'row'), 'col')
- output 4: float32 [20480], P(('part', 'col'))
- output 5: bfloat16 [20480, 5120], P(('part', 'col', 'row'), 'dep')
- output 6: float32 [5120], P(('part', 'dep'))
- output 7: float32 [5120], P(('part', 'dep'))
- output 8: float32 [5120], P(('part', 'dep'))
All inputs are finite; a program needn't handle non-finite values.
Results may differ from the reference program's by a relative error of at most 0.0017.
Values are sent between devices in bfloat16 or wider.
A program may use at most 1 GiB of HBM per device.

```python
import jax
import jax.numpy as jnp
from jax import lax

TOKENS = 4096
D_MODEL = 5120
D_FF = 20480

BLOCK_ROWS = min(TOKENS, 512)
N_BLOCKS = TOKENS // BLOCK_ROWS
LN_EPS = 1e-5
GELU_K = 0.7978845608028654
GELU_C = 0.044715
TWO_PI = 6.283185307179586


def setup_inputs(seed: int = 0, part: int = 0) -> dict:
    shared_root, part_root = jax.random.split(jax.random.key(seed))
    part_keys = jax.random.split(jax.random.fold_in(part_root, part), 4)
    shared_keys = jax.random.split(shared_root, 6)
    col_pos = jnp.arange(D_MODEL, dtype=jnp.float32) / D_MODEL
    col_phase = jax.random.uniform(part_keys[0], (), jnp.float32, 0.0, TWO_PI)
    col_mean = 1.5 * jnp.sin(TWO_PI * col_pos + col_phase) + 0.5 * jax.random.normal(part_keys[1], (D_MODEL,), jnp.float32)
    x_vals = jax.random.normal(part_keys[2], (TOKENS, D_MODEL), jnp.float32) + col_mean
    g_vals = jax.random.normal(part_keys[3], (TOKENS, D_MODEL), jnp.float32)
    return {
        "x_in": x_vals.astype(jnp.bfloat16),
        "ln_scale": 1.0 + 0.3 * jax.random.normal(shared_keys[0], (D_MODEL,), jnp.float32),
        "ln_shift": 0.5 * jax.random.normal(shared_keys[1], (D_MODEL,), jnp.float32),
        "w_up": (jax.random.normal(shared_keys[2], (D_MODEL, D_FF), jnp.float32) * D_MODEL ** -0.5).astype(jnp.bfloat16),
        "b_up": (0.5 * jax.random.normal(shared_keys[3], (D_FF,), jnp.float32)).astype(jnp.bfloat16),
        "w_down": (jax.random.normal(shared_keys[4], (D_FF, D_MODEL), jnp.float32) * D_FF ** -0.5).astype(jnp.bfloat16),
        "b_down": (0.5 * jax.random.normal(shared_keys[5], (D_MODEL,), jnp.float32)).astype(jnp.bfloat16),
        "y_grad": g_vals.astype(jnp.bfloat16),
    }


def gelu_tanh(pre_act):
    inner_arg = GELU_K * (pre_act + GELU_C * pre_act * (pre_act * pre_act))
    return 0.5 * pre_act * (1.0 + jnp.tanh(inner_arg))


def gelu_slope(pre_act):
    squared = pre_act * pre_act
    tanh_val = jnp.tanh(GELU_K * (pre_act + GELU_C * pre_act * squared))
    return 0.5 * (1.0 + tanh_val) + 0.5 * pre_act * (1.0 - tanh_val * tanh_val) * GELU_K * (1.0 + 3.0 * GELU_C * squared)


def block_pass(x_blk, g_blk, ln_scale, ln_shift, w_up, b_up, w_down, b_down):
    x_float = x_blk.astype(jnp.float32)
    mean_row = jnp.sum(x_float, axis=1, keepdims=True) / D_MODEL
    var_row = jnp.sum(x_float * x_float, axis=1, keepdims=True) / D_MODEL - mean_row * mean_row
    inv_std = lax.rsqrt(var_row + LN_EPS)
    x_hat = (x_float - mean_row) * inv_std
    normed = (x_hat * ln_scale + ln_shift).astype(jnp.bfloat16)
    pre_act = jnp.dot(normed, w_up, preferred_element_type=jnp.float32) + b_up.astype(jnp.float32)
    hidden = gelu_tanh(pre_act).astype(jnp.bfloat16)
    out_sum = jnp.dot(hidden, w_down, preferred_element_type=jnp.float32)
    y_blk = (x_float + out_sum + b_down.astype(jnp.float32)).astype(jnp.bfloat16)
    g_float = g_blk.astype(jnp.float32)
    w_down_part = jnp.dot(hidden.T, g_blk, preferred_element_type=jnp.float32)
    hid_grad = jnp.dot(g_blk, w_down.T, preferred_element_type=jnp.float32)
    pre_grad = hid_grad * gelu_slope(pre_act)
    pre_lowp = pre_grad.astype(jnp.bfloat16)
    w_up_part = jnp.dot(normed.T, pre_lowp, preferred_element_type=jnp.float32)
    norm_grad = jnp.dot(pre_lowp, w_up.T, preferred_element_type=jnp.float32)
    xhat_grad = norm_grad * ln_scale
    mean_one = jnp.sum(xhat_grad, axis=1, keepdims=True) / D_MODEL
    mean_two = jnp.sum(xhat_grad * x_hat, axis=1, keepdims=True) / D_MODEL
    dx_blk = (g_float + inv_std * (xhat_grad - mean_one - x_hat * mean_two)).astype(jnp.bfloat16)
    part_sums = (w_up_part, jnp.sum(pre_grad, axis=0), w_down_part, jnp.sum(g_float, axis=0), jnp.sum(norm_grad * x_hat, axis=0), jnp.sum(norm_grad, axis=0))
    return y_blk, dx_blk, part_sums


def reference(x_in, ln_scale, ln_shift, w_up, b_up, w_down, b_down, y_grad):
    x_blocks = x_in.reshape(N_BLOCKS, BLOCK_ROWS, D_MODEL)
    g_blocks = y_grad.reshape(N_BLOCKS, BLOCK_ROWS, D_MODEL)

    def scan_step(acc_sums, blk_pair):
        y_blk, dx_blk, part_sums = block_pass(blk_pair[0], blk_pair[1], ln_scale, ln_shift, w_up, b_up, w_down, b_down)
        new_sums = tuple(acc_val + add_val for acc_val, add_val in zip(acc_sums, part_sums))
        return new_sums, (y_blk, dx_blk)

    zero_sums = (jnp.zeros((D_MODEL, D_FF), jnp.float32), jnp.zeros((D_FF,), jnp.float32), jnp.zeros((D_FF, D_MODEL), jnp.float32), jnp.zeros((D_MODEL,), jnp.float32), jnp.zeros((D_MODEL,), jnp.float32), jnp.zeros((D_MODEL,), jnp.float32))
    total_sums, out_blocks = lax.scan(scan_step, zero_sums, (x_blocks, g_blocks))
    return (out_blocks[0].reshape(TOKENS, D_MODEL), out_blocks[1].reshape(TOKENS, D_MODEL), total_sums[0].astype(jnp.bfloat16), total_sums[1], total_sums[2].astype(jnp.bfloat16), total_sums[3], total_sums[4], total_sums[5])
```

```python
import jax
import jax.numpy as jnp
from jax import lax
from jax.sharding import PartitionSpec as P


LN_EPS = 1e-5
GELU_K = 0.7978845608028654
GELU_C = 0.044715
SWAP = ((0, 1), (1, 0))
F32 = jnp.float32
BF16 = jnp.bfloat16


def gelu_tanh(pre_act):
    inner_arg = GELU_K * (pre_act + GELU_C * pre_act * (pre_act * pre_act))
    return 0.5 * pre_act * (1.0 + jnp.tanh(inner_arg))


def gelu_slope(pre_act):
    squared = pre_act * pre_act
    tanh_val = jnp.tanh(GELU_K * (pre_act + GELU_C * pre_act * squared))
    return 0.5 * (1.0 + tanh_val) + 0.5 * pre_act * (1.0 - tanh_val * tanh_val) * GELU_K * (1.0 + 3.0 * GELU_C * squared)


def swap(val, axis):
    return lax.ppermute(val, axis, SWAP)


def ordered(idx, mine, other, axis):
    return jnp.where(idx == 0, jnp.concatenate([mine, other], axis), jnp.concatenate([other, mine], axis))


def dot_nn(lhs, rhs):
    return lax.dot_general(lhs, rhs, (((1,), (0,)), ((), ())), preferred_element_type=F32)


def dot_nt(lhs, rhs):
    return lax.dot_general(lhs, rhs, (((1,), (1,)), ((), ())), preferred_element_type=F32)


def dot_tn(lhs, rhs):
    return lax.dot_general(lhs, rhs, (((0,), (0,)), ((), ())), preferred_element_type=F32)


def solution(mesh):
    assert mesh.shape["row"] == 2 and mesh.shape["col"] == 2 and mesh.shape["dep"] == 2
    tok_spec = P(("part", "row", "col"), "dep")
    vec_dep = P("dep")
    part_dep = P(("part", "dep"))
    in_specs = (tok_spec, vec_dep, vec_dep, P(("dep", "row"), "col"), P("col"), P(("col", "row"), "dep"), vec_dep, tok_spec)
    out_specs = (tok_spec, tok_spec, P(("part", "dep", "row"), "col"), P(("part", "col")), P(("part", "col", "row"), "dep"), part_dep, part_dep, part_dep)

    def layer(x_in, ln_scale, ln_shift, w_up, b_up, w_down, b_down, y_grad):
        row = lax.axis_index("row")
        dep = lax.axis_index("dep")
        half_d = x_in.shape[1]
        row_width = half_d * 2
        quarter = w_up.shape[1] // 2
        own_f = quarter // 2
        up_rows = w_up.shape[0]

        last = [None]

        def after(vals):
            if last[0] is None:
                return vals
            return lax.optimization_barrier((vals, last[0]))[0]

        def step(fn, *vals):
            out = fn(*after(vals))
            last[0] = out[0] if isinstance(out, tuple) else out
            return out

        def launch(val, axis):
            val = after(val)
            return lax.ppermute(val, axis, SWAP)

        a_mine, a_peer, g_mine, g_peer = {}, {}, {}, {}
        hid_grad, pre_half, pre, hidden, pre_grad, pre_lowp = {}, {}, {}, {}, {}, {}
        out_came, out_chip, norm_came, norm_chip = {}, {}, {}, {}
        far_at = (0, (1 - row) * quarter + (1 - dep) * own_f)
        near_at = (0, (1 - row) * quarter + dep * own_f)
        pass_at = (0, row * quarter + (1 - dep) * own_f)
        keep_at = (0, row * quarter + dep * own_f)
        up_block = (up_rows, own_f)

        g_mine["O"] = y_grad
        g_mine["X"] = launch(y_grad, "col")
        up_far = launch(step(lambda w: lax.dynamic_slice(w, far_at, up_block), w_up), "row")

        def stats_of(x):
            x_float = x.astype(F32)
            return jnp.stack([jnp.sum(x_float, axis=1), jnp.sum(x_float * x_float, axis=1)], axis=0)

        row_stats = step(stats_of, x_in)
        row_stats = row_stats + swap(row_stats, "dep")
        mean_row = (row_stats[0] / row_width)[:, None]
        var_row = (row_stats[1] / row_width)[:, None] - mean_row * mean_row
        inv_std = lax.rsqrt(var_row + LN_EPS)
        normed = step(lambda x, m, i: ((x.astype(F32) - m) * i * ln_scale + ln_shift).astype(BF16), x_in, mean_row, inv_std)
        a_mine["O"] = normed
        a_mine["Y"] = launch(normed, "row")
        a_mine["X"] = launch(normed, "col")
        up_near = launch(step(lambda w: lax.dynamic_slice(w, near_at, up_block), w_up), "row")
        g_peer["O"] = launch(y_grad, "dep")
        down_peer = launch(step(lambda w: lax.dynamic_slice(w, ((1 - dep) * own_f, 0), (own_f, half_d)), w_down), "dep")
        up_pass = launch(step(lambda w: lax.dynamic_slice(w, pass_at, up_block), w_up), "dep")
        a_peer["O"] = launch(normed, "dep")
        down_own = step(lambda w: lax.dynamic_slice(w, (dep * own_f, 0), (own_f, half_d)), w_down)
        bias = lax.dynamic_slice(b_up, (row * quarter + dep * own_f,), (own_f,)).astype(F32)

        def run_hid_grad(k):
            part = step(dot_nt, g_mine[k], down_own)
            hid_grad[k] = step(lambda g, w, p: dot_nt(g, w) + p, g_peer[k], down_peer, part)

        def run_pre_half(k):
            pre_half[k] = step(dot_nn, a_peer[k], up_peer)

        def run_pre(k):
            def body(act, weight, half):
                total = dot_nn(act, weight) + half + bias
                return gelu_tanh(total).astype(BF16), total

            hidden[k], pre[k] = step(body, a_mine[k], up_own, pre_half[k])

        def run_pre_grad(k):
            def body(grad, act):
                full = grad * gelu_slope(act)
                return full.astype(BF16), full

            pre_lowp[k], pre_grad[k] = step(body, hid_grad[k], pre[k])

        def out_peer(k):
            out_came[k] = launch(step(dot_nn, hidden[k], down_peer), "dep")

        def out_own(k):
            out_chip[k] = step(lambda h, w, c: dot_nn(h, w) + c, hidden[k], down_own, out_came[k])

        def norm_peer(k):
            norm_came[k] = launch(step(dot_nt, pre_lowp[k], up_peer), "dep")

        def norm_own(k):
            norm_chip[k] = step(lambda h, w, c: dot_nt(h, w) + c, pre_lowp[k], up_own, norm_came[k])

        run_hid_grad("O")
        g_peer["X"] = launch(g_mine["X"], "dep")
        run_hid_grad("X")
        far_here = launch(up_far, "dep")
        up_peer = step(lambda kept, came: ordered(row, kept, came, 0), up_pass, far_here)
        run_pre_half("O")
        a_peer["X"] = launch(a_mine["X"], "dep")
        run_pre_half("X")
        a_peer["Y"] = launch(a_mine["Y"], "dep")
        a_mine["D"] = launch(a_mine["Y"], "col")
        run_pre_half("Y")
        a_peer["D"] = launch(a_mine["D"], "dep")
        run_pre_half("D")
        up_own = step(lambda w, came: ordered(row, lax.dynamic_slice(w, keep_at, up_block), came, 0), w_up, up_near)
        g_mine["Y"] = launch(y_grad, "row")
        g_mine["D"] = launch(g_mine["X"], "row")
        run_pre("D")
        out_peer("D")
        run_pre("Y")
        out_peer("Y")
        out_own("D")
        out_diag = launch(out_chip["D"], "col")
        out_own("Y")
        run_pre("X")
        run_pre("O")
        out_peer("X")
        out_peer("O")
        g_peer["Y"] = launch(g_mine["Y"], "dep")
        run_pre_grad("X")
        run_pre_grad("O")
        out_own("O")
        run_hid_grad("Y")
        g_peer["D"] = launch(g_mine["D"], "dep")
        run_pre_grad("Y")
        norm_peer("Y")
        run_hid_grad("D")
        run_pre_grad("D")
        norm_peer("D")
        b_up_own = step(lambda p: sum(jnp.sum(v, axis=0) for v in p.values()), pre_grad)
        b_up_came = launch(b_up_own, "dep")
        norm_own("Y")
        b_up_near = step(lambda own, came: ordered(dep, own, came, 0), b_up_own, b_up_came)
        b_up_far = launch(b_up_near, "row")
        norm_peer("X")
        norm_own("D")
        norm_diag = launch(norm_chip["D"], "col")
        out_own("X")
        out_x = launch(out_chip["X"], "col")
        out_y = launch(step(jnp.add, out_chip["Y"], out_diag), "row")
        norm_own("X")
        norm_x = launch(norm_chip["X"], "col")
        norm_peer("O")

        def token_sum(lhs, rhs):
            total = step(dot_tn, lhs["O"], rhs["O"])
            for k in "XY":
                total = step(lambda a, b, t: dot_tn(a, b) + t, lhs[k], rhs[k], total)
            return step(lambda a, b, t: (dot_tn(a, b) + t).astype(BF16), lhs["D"], rhs["D"], total)

        down_g_came = launch(token_sum(hidden, g_peer), "dep")
        norm_own("O")
        down_g_own = token_sum(hidden, g_mine)
        norm_y = launch(step(jnp.add, norm_chip["Y"], norm_diag), "row")
        up_g_came = launch(token_sum(a_peer, pre_lowp), "dep")
        up_g_own = token_sum(a_mine, pre_lowp)

        def up_rows_of(own, came, row_idx):
            at = (row_idx * up_rows, 0)
            return ordered(dep, lax.dynamic_slice(own, at, up_block), lax.dynamic_slice(came, at, up_block), 1)

        up_g_far = launch(step(lambda own, came: up_rows_of(own, came, 1 - row), up_g_own, up_g_came), "row")
        up_g_near = step(lambda own, came: up_rows_of(own, came, row), up_g_own, up_g_came)
        w_down_grad = step(lambda own, came: ordered(dep, own, came, 0), down_g_own, down_g_came)
        x_float = x_in.astype(F32)
        y_out = step(lambda x, c, n, y: (x.astype(F32) + ((c + n) + y) + b_down.astype(F32)).astype(BF16), x_in, out_chip["O"], out_x, out_y)
        norm_grad = step(lambda c, n, y: (c + n) + y, norm_chip["O"], norm_x, norm_y)
        w_up_grad = ordered(row, up_g_near, up_g_far, 1)

        b_up_grad = ordered(row, b_up_near, b_up_far, 0)
        g_float = y_grad.astype(F32)
        b_down_grad = sum(jnp.sum(g.astype(F32), axis=0) for g in g_mine.values())

        x_hat = (x_float - mean_row) * inv_std
        value = norm_grad * ln_scale
        grad_stats = jnp.stack([jnp.sum(value, axis=1), jnp.sum(value * x_hat, axis=1)], axis=0)
        grad_stats = grad_stats + swap(grad_stats, "dep")
        mean_one = (grad_stats[0] / row_width)[:, None]
        mean_two = (grad_stats[1] / row_width)[:, None]
        x_grad = (g_float + inv_std * (value - mean_one - x_hat * mean_two)).astype(BF16)
        gain_sums = jnp.stack([jnp.sum(norm_grad * x_hat, axis=0), jnp.sum(norm_grad, axis=0)])
        gain_sums = gain_sums + swap(gain_sums, "col")
        gain_sums = gain_sums + swap(gain_sums, "row")
        return (y_out, x_grad, w_up_grad, b_up_grad, w_down_grad, b_down_grad, gain_sums[0], gain_sums[1])

    mapped = jax.shard_map(layer, mesh=mesh, in_specs=in_specs, out_specs=out_specs, check_vma=False)

    def run(*args):
        jax.eval_shape(mapped, *args)
        return mapped(*args)

    return run
```
